32 devices in a mesh: blk: 8 (over y, x, core), uly: 1, dp: 4 (over z).
Axes of the slice: x: 2, y: 2, z: 4, core: 2. Of those that a mesh axis runs over, the one named last changes fastest.
Arguments:
- short_tokens: bfloat16 [32, 1024, 4096], P(('blk', 'dp'), 'uly'), may hold values from -150 to 150, as said below
- short_segments: int32 [32, 1024], P(('blk', 'dp')), may hold values from 0 to 3, never falling along the last dimension, each value on 1 to 512 neighbouring positions
- long_tokens: bfloat16 [4, 3072, 4096], P('dp', 'blk'), may hold values from -150 to 150, as said below
- long_lengths: int32 [4], P('dp'), may hold values from 768 to 3072
- w_query: bfloat16 [4096, 2048], P(('blk', 'dp'), 'uly'), may hold values from -0.09375 to 0.09375
- w_key: bfloat16 [4096, 512], P(('blk', 'dp'), 'uly'), may hold values from -0.09375 to 0.09375
- w_value: bfloat16 [4096, 512], P(('blk', 'dp'), 'uly'), may hold values from -0.09375 to 0.09375
Outputs:
- short_out: bfloat16 [32, 1024, 2048], P(('blk', 'dp'), 'uly')
- long_out: bfloat16 [4, 3072, 2048], P('dp', 'blk', 'uly')
The draws below stay inside these ranges and needn't reach their ends.
Inputs may be any that keep to these rules, and one draw needn't show every extreme that they name: `short_tokens`: activations of the short bucket. `long_tokens`: activations of the long bucket; rows at or after a sequence's length are padding. `short_segments`: document numbers never fall along a sequence. `long_lengths`: a long sequence occupies positions 0 to its length - 1 of its 3072 slots.
All inputs are finite; a program needn't handle non-finite values.
Results may differ from the reference program's by a relative error of at most 0.012.
The reference program's roundings to bfloat16 on the way count: a program that leaves them out, or rounds other values in their place, can miss the bound.
Values may be sent and summed in bfloat16 or wider, within the bound.
A program may use at most 128 MiB of HBM per device.

```python
import math
import jax
import jax.numpy as jnp
import numpy as np
from jax import lax

D = 4096
HQ = 16
HK = 4
HD = 128
LS = 1024
NS = 32
NL = 4
LL = 3072


def token_rows(key, shape):
    base = jnp.clip(jax.random.normal(key, shape, jnp.float32), -6.0, 6.0)
    return base.astype(jnp.bfloat16)


def draw_short_tokens(key, part):
    return token_rows(jax.random.fold_in(key, 101), (NS, LS, D))


def draw_long_tokens(key, part):
    return token_rows(jax.random.fold_in(key, 202), (NL, LL, D))


def plant(values, stream_key, low, largest):
    place = [jax.random.randint(jax.random.fold_in(stream_key, axis), (), 0, length) for axis, length in enumerate(values.shape)]
    longest = values.shape.index(max(values.shape))
    neighbour = place[:longest] + [(place[longest] + 1) % values.shape[longest]] + place[longest + 1:]
    return values.at[tuple(place)].set(low).at[tuple(neighbour)].set(largest)


def levels(rng, dims, shards, least, top_value):
    def one(dim, blocks):
        heights = jax.random.uniform(jax.random.fold_in(jax.random.fold_in(rng, 6), dim), (blocks,), jnp.float32, least / len(shards), top_value / len(shards))
        return jnp.repeat(jnp.exp(heights), dims[dim] // blocks).reshape((-1,) + (1,) * (len(dims) - dim - 1))

    loudness = one(*shards[0])
    for cut in shards[1:]:
        loudness = loudness * one(*cut)
    return loudness


def length_profile(number_of, total, most, lean):
    weights = [(1 << 20) // math.isqrt(grade ** lean) + 1 for grade in range(2, number_of + 1)]
    spare, counts = total - most - (number_of - 1), [1] * (number_of - 1)
    while spare > 0:
        movable = [i for i in range(number_of - 1) if counts[i] < most]
        whole, remaining = sum([weights[i] for i in movable]), spare
        for i in movable:
            extra = min(most - counts[i], max(1, remaining * weights[i] // whole), spare)
            counts[i] = counts[i] + extra
            spare = spare - extra
    return np.array([most] + counts)


def uneven(own_key, number_of, total, most, lean):
    if number_of == 2:
        one = jax.random.randint(own_key, (), max(1, total - most), min(most, total - 1) + 1)
        return jnp.stack([one, total - one])
    lengths = jnp.asarray(length_profile(number_of, total, most, lean), jnp.int32)
    twos = (number_of - 1) // 2
    donor, receiver = lengths[1:1 + 2 * twos:2], lengths[2:2 + 2 * twos:2]
    room = jnp.minimum(donor - 1, most - receiver)
    shifted = jax.random.randint(jax.random.fold_in(own_key, 1), (twos,), 0, 1 << 20) % (room + 1)
    lengths = lengths.at[1:1 + 2 * twos:2].set(donor - shifted).at[2:2 + 2 * twos:2].set(receiver + shifted)
    return lengths[jax.random.permutation(jax.random.fold_in(own_key, 2), number_of)]


def gaussian(own_key, extent, width, bound, split=(), kind=jnp.bfloat16):
    factor_of = levels(own_key, extent, split, -0.22, 0.18) if split else 1.0
    drawn = jax.random.normal(own_key, extent, jnp.float32) * width * factor_of
    return jnp.minimum(jnp.maximum(drawn, -bound), bound).astype(kind)


def setup_inputs(seed: int = 0) -> dict:
    keys = jax.random.split(jax.random.key(seed), 8)
    short_tokens = draw_short_tokens(jax.random.fold_in(keys[7], 71), 0)
    short_segments = jax.vmap(lambda own: jnp.searchsorted(jnp.cumsum(uneven(own, 4, LS, LS // 2, 1)), jnp.arange(LS), side="right"))(jax.random.split(keys[1], NS)).reshape((NS, LS)).astype(jnp.int32)
    long_tokens = draw_long_tokens(jax.random.fold_in(keys[7], 71), 0)
    long_lengths = plant(jax.random.randint(keys[3], (NL,), LL // 4, LL + 1), jax.random.fold_in(keys[3], 1), LL // 4, LL).astype(jnp.int32)
    w_query = gaussian(keys[4], (D, HQ * HD), D ** -0.5, 0.09375, ((0, 32),))
    w_key = gaussian(keys[5], (D, HK * HD), D ** -0.5, 0.09375, ((0, 32),))
    w_value = gaussian(keys[6], (D, HK * HD), D ** -0.5, 0.09375, ((0, 32),))
    return {"short_tokens": short_tokens, "short_segments": short_segments, "long_tokens": long_tokens, "long_lengths": long_lengths, "w_query": w_query, "w_key": w_key, "w_value": w_value}


masked_score = -1e+30

def rounded_wide(array):
    return lax.optimization_barrier(array.astype(jnp.bfloat16)).astype(jnp.float32)

def project(rows, weight):
    return jnp.dot(rows, weight, preferred_element_type=jnp.float32)

def attention(queries, key_rows, value_rows, visible_rows):
    seq_len = key_rows.shape[0]
    block_rows = min(512, seq_len)
    group_size = HQ // HK
    key_heads = key_rows.reshape(seq_len, HK, HD)
    value_heads = value_rows.reshape(seq_len, HK, HD)
    outputs = []
    for block_index in range(seq_len // block_rows):
        first_row = block_index * block_rows
        query_heads = queries[first_row:first_row + block_rows].reshape(block_rows, HK, group_size, HD)
        visible = visible_rows(first_row, block_rows)
        scores = jnp.einsum('bhgd,khd->hgbk', query_heads, key_heads) * (1.0 / math.sqrt(HD))
        scores = jnp.where(visible, scores, masked_score)
        row_max = lax.optimization_barrier(jnp.max(scores, axis=-1, keepdims=True))
        exponentials = jnp.where(visible, jnp.exp(scores - row_max), 0.0)
        totals = lax.optimization_barrier(jnp.sum(exponentials, axis=-1))
        mixed = jnp.einsum('hgbk,khd->hgbd', rounded_wide(exponentials), value_heads)
        mixed = mixed / totals[..., None]
        outputs.append(jnp.transpose(mixed, (2, 0, 1, 3)).reshape(block_rows, HQ * HD))
    return jnp.concatenate(outputs, axis=0)

def reference(short_tokens, short_segments, long_tokens, long_lengths, w_query, w_key, w_value):

    def one_short(inputs):
        rows, segments = inputs
        queries = rounded_wide(project(rows, w_query))
        key_rows = rounded_wide(project(rows, w_key))
        value_rows = rounded_wide(project(rows, w_value))
        positions = jnp.arange(rows.shape[0], dtype=jnp.int32)

        def visible_rows(first_row, block_rows):
            query_pos = positions[first_row:first_row + block_rows]
            query_seg = segments[first_row:first_row + block_rows]
            return (positions[None, :] <= query_pos[:, None]) & (segments[None, :] == query_seg[:, None])
        mixed = attention(queries, key_rows, value_rows, visible_rows)
        return mixed.astype(jnp.bfloat16)

    def one_long(inputs):
        rows, length = inputs
        queries = rounded_wide(project(rows, w_query))
        key_rows = rounded_wide(project(rows, w_key))
        value_rows = rounded_wide(project(rows, w_value))
        positions = jnp.arange(rows.shape[0], dtype=jnp.int32)

        def visible_rows(first_row, block_rows):
            query_pos = positions[first_row:first_row + block_rows]
            return (positions[None, :] <= query_pos[:, None]) & (positions[None, :] < length)
        mixed = attention(queries, key_rows, value_rows, visible_rows)
        mixed = jnp.where(positions[:, None] < length, mixed, 0.0)
        return mixed.astype(jnp.bfloat16)
    short_out = lax.map(one_short, (short_tokens, short_segments))
    long_out = lax.map(one_long, (long_tokens, long_lengths))
    return (short_out, long_out)
```

```python
import functools
import math

import jax
import jax.numpy as jnp
from jax import lax
from jax.experimental import pallas as pl
from jax.experimental.pallas import tpu as pltpu
from jax.sharding import PartitionSpec as P

HD = 128
LONGEST_DOCUMENT = 512

masked_score = -1e30
exp2_factor = math.log2(math.e) / math.sqrt(HD)


def raw_scores(queries, keys):
    return lax.dot_general(
        queries, keys, (((1,), (1,)), ((), ())), preferred_element_type=jnp.float32
    )


def short_kernel(block_rows, col_ref, row_ref, q_ref, k_ref, v_ref, out_ref, bias_ref):
    seq_len = q_ref.shape[0]

    def window(first_row):
        return max(0, first_row - LONGEST_DOCUMENT), first_row + block_rows

    @pl.when(pl.program_id(0) == 0)
    def _():
        for first_row in range(0, seq_len, block_rows):
            low, high = window(first_row)
            shape = (block_rows, high - low)
            query_pos = first_row + lax.broadcasted_iota(jnp.int32, shape, 0)
            key_pos = low + lax.broadcasted_iota(jnp.int32, shape, 1)
            visible = (key_pos <= query_pos) & (
                col_ref[first_row : first_row + block_rows, :] == row_ref[:, low:high]
            )
            bias_ref[first_row : first_row + block_rows, low:high] = jnp.where(
                visible, 0.0, masked_score
            )

    for first_row in range(0, seq_len, block_rows):
        low, high = window(first_row)
        rows = slice(first_row, first_row + block_rows)
        scores = raw_scores(q_ref[rows, :], k_ref[low:high, :]) + bias_ref[rows, low:high]
        row_max = jnp.max(scores, axis=-1, keepdims=True)
        exponentials = jnp.exp2((scores - row_max) * exp2_factor)
        totals = jnp.sum(exponentials, axis=-1, keepdims=True)
        mixed = jnp.dot(
            exponentials.astype(jnp.bfloat16),
            v_ref[low:high, :],
            preferred_element_type=jnp.float32,
        )
        out_ref[rows, :] = (mixed / totals).astype(jnp.bfloat16)


def short_attention(projected, segments, heads, kv_heads):
    seq_len = projected.shape[0]
    group = heads // kv_heads
    block_rows = math.gcd(seq_len, 256)
    return pl.pallas_call(
        functools.partial(short_kernel, block_rows),
        grid=(heads,),
        in_specs=[
            pl.BlockSpec((seq_len, 1), lambda h: (0, 0)),
            pl.BlockSpec((1, seq_len), lambda h: (0, 0)),
            pl.BlockSpec((seq_len, HD), lambda h: (0, h)),
            pl.BlockSpec((seq_len, HD), lambda h: (0, heads + h // group)),
            pl.BlockSpec((seq_len, HD), lambda h: (0, heads + kv_heads + h // group)),
        ],
        out_specs=pl.BlockSpec((seq_len, HD), lambda h: (0, h)),
        out_shape=jax.ShapeDtypeStruct((seq_len, heads * HD), jnp.bfloat16),
        scratch_shapes=[pltpu.VMEM((seq_len, seq_len), jnp.float32)],
        cost_estimate=pl.CostEstimate(
            flops=4 * heads * seq_len * seq_len * HD,
            bytes_accessed=4 * seq_len * heads * HD,
            transcendentals=heads * seq_len * seq_len,
        ),
        compiler_params=pltpu.CompilerParams(dimension_semantics=("arbitrary",)),
    )(segments[:, None], segments[None, :], projected, projected, projected)


def long_kernel(key_rows, info_ref, q_ref, k_ref, v_ref, out_ref):
    long_count = q_ref.shape[0]
    first_pos = info_ref[0]
    long_len = info_ref[1]
    queries = q_ref[...]
    query_pos = first_pos + lax.broadcasted_iota(jnp.int32, (long_count, 1), 0)
    last_key = jnp.minimum(query_pos, long_len - 1)

    def update(block, states, masked):
        running_max, running_sum, accumulated = states
        start = pl.multiple_of(block * key_rows, key_rows)
        scores = raw_scores(queries, k_ref[pl.ds(start, key_rows), :])
        if masked:
            key_pos = start + lax.broadcasted_iota(jnp.int32, (long_count, key_rows), 1)
            scores = jnp.where(key_pos <= last_key, scores, masked_score)
        new_max = jnp.maximum(running_max, jnp.max(scores, axis=-1, keepdims=True))
        rescale = jnp.exp2((running_max - new_max) * exp2_factor)
        exponentials = jnp.exp2((scores - new_max) * exp2_factor)
        running_sum = running_sum * rescale + jnp.sum(exponentials, axis=-1, keepdims=True)
        accumulated = accumulated * rescale + jnp.dot(
            exponentials.astype(jnp.bfloat16),
            v_ref[pl.ds(start, key_rows), :],
            preferred_element_type=jnp.float32,
        )
        return new_max, running_sum, accumulated

    @pl.when(first_pos >= long_len)
    def _():
        out_ref[...] = jnp.zeros_like(out_ref)

    @pl.when(first_pos < long_len)
    def _():
        whole = jnp.minimum(first_pos + 1, long_len) // key_rows
        used = (jnp.minimum(first_pos + long_count, long_len) + key_rows - 1) // key_rows
        states = (
            jnp.full((long_count, 1), masked_score, jnp.float32),
            jnp.zeros((long_count, 1), jnp.float32),
            jnp.zeros((long_count, HD), jnp.float32),
        )
        states = lax.fori_loop(0, whole, lambda i, s: update(i, s, False), states)
        states = lax.fori_loop(whole, used, lambda i, s: update(i, s, True), states)
        running_max, running_sum, accumulated = states
        mixed = jnp.where(query_pos < long_len, accumulated / running_sum, 0.0)
        out_ref[...] = mixed.astype(jnp.bfloat16)


def long_attention(queries, kv_rows, first_pos, long_len, kv_heads):
    long_count = queries.shape[0]
    heads = queries.shape[1] // HD
    total_rows = kv_rows.shape[0]
    group = heads // kv_heads
    key_rows = math.gcd(total_rows, 768)
    return pl.pallas_call(
        functools.partial(long_kernel, key_rows),
        grid_spec=pltpu.PrefetchScalarGridSpec(
            num_scalar_prefetch=1,
            grid=(heads,),
            in_specs=[
                pl.BlockSpec((long_count, HD), lambda h, info: (0, h)),
                pl.BlockSpec((total_rows, HD), lambda h, info: (0, h // group)),
                pl.BlockSpec((total_rows, HD), lambda h, info: (0, kv_heads + h // group)),
            ],
            out_specs=pl.BlockSpec((long_count, HD), lambda h, info: (0, h)),
        ),
        out_shape=jax.ShapeDtypeStruct((long_count, heads * HD), jnp.bfloat16),
        cost_estimate=pl.CostEstimate(
            flops=4 * heads * long_count * total_rows * HD,
            bytes_accessed=4 * total_rows * kv_heads * HD,
            transcendentals=heads * long_count * total_rows,
        ),
        compiler_params=pltpu.CompilerParams(dimension_semantics=("arbitrary",)),
    )(jnp.stack([first_pos, long_len]), queries, kv_rows, kv_rows)


def project(rows, weight):
    return jnp.dot(rows, weight, preferred_element_type=jnp.float32).astype(jnp.bfloat16)


def local(short_tokens, short_segments, long_tokens, long_lengths, w_query, w_key, w_value):
    short_rows = short_tokens[0]
    long_rows = long_tokens[0]
    long_count = long_rows.shape[0]
    query_cols = w_query.shape[1]
    heads, kv_heads = query_cols // HD, w_key.shape[1] // HD
    weights = lax.all_gather(
        jnp.concatenate([w_query, w_key, w_value], axis=1), ("blk", "dp"), axis=0, tiled=True
    )
    kv_long = project(long_rows, weights[:, query_cols:])
    kv_whole = lax.all_gather(kv_long, "blk", axis=0, tiled=True)
    whole_rows = lax.all_gather(short_rows, "uly", axis=0, tiled=True)
    short_projected = project(whole_rows, weights)
    query_long = project(long_rows, weights[:, :query_cols])
    attended = short_attention(short_projected, short_segments[0], heads, kv_heads)
    short_back = lax.all_to_all(attended, "uly", split_axis=0, concat_axis=1, tiled=True)
    first_pos = lax.axis_index("blk").astype(jnp.int32) * long_count
    mixed = long_attention(query_long, kv_whole, first_pos, long_lengths[0], kv_heads)
    return short_back[None], mixed[None]


MESH = pl.DeviceIdType.MESH


def fused_kernel(
    dims, len_ref, segcol_in, segrow_in, short_ref, long_ref, wq_ref, wk_ref, wv_ref,
    short_out, long_out,
    x, w, proj, far_kv, bias, staged, segcol, segrow,
    z_send, z_recv, x_send, x_recv, y_send, y_recv, dx_send, dx_recv, dy_send, dy_recv,
    own_sem, sib_send, sib_recv, tok_sem, tok_send, tok_recv, seg_sem, seg_send, seg_recv,
    kv_send, kv_recv, out_sem, out_send, out_recv, total, highest,
):
    planes, short_len, long_count, groups, pairs, rows_step = dims
    per_group = 1 + pairs
    steps = groups * per_group
    plane_first = steps - 1
    both_short, both_long = 2 * short_len, 2 * long_count
    half_q, half_kv = groups * pairs * 2 * HD, groups * HD

    b, z = lax.axis_index("blk"), lax.axis_index("dp")
    core, chip = b % 2, b // 2
    cx, cy = chip % 2, chip // 2
    sib = b + 1 - 2 * core
    bx = b + 2 - 4 * cx
    by = b + 4 - 8 * cy
    bd = bx + by - b
    chip_x, chip_y = bx // 2, by // 2

    def z_at(k):
        return (z + k) % planes

    def remote(src, dst, send, recv, blk, dp=None):
        where = {"blk": blk} if dp is None else {"dp": dp}
        return pltpu.make_async_remote_copy(
            src_ref=src, dst_ref=dst, send_sem=send, recv_sem=recv,
            device_id=where, device_id_type=MESH,
        )

    barrier = pltpu.get_barrier_semaphore()
    for peer in (sib, bx, by, bd):
        pl.semaphore_signal(barrier, inc=1, device_id={"blk": peer}, device_id_type=MESH)
    for k in range(1, planes):
        pl.semaphore_signal(barrier, inc=1, device_id={"dp": z_at(k)}, device_id_type=MESH)
    pl.semaphore_wait(barrier, 4 + planes - 1)

    def weight_parts(p, half):
        g, r = p // per_group, p % per_group
        if r == 0:
            return ((wk_ref, half * half_kv + g * HD), (wv_ref, half * half_kv + g * HD))
        q = half * half_q + (g * pairs + r - 1) * 2 * HD
        return ((wq_ref, q), (wq_ref, q + HD))

    def own_weight(p, part):
        ref, col = weight_parts(p, core)[part]
        return pltpu.make_async_copy(
            ref.at[:, pl.ds(pl.multiple_of(col, HD), HD)],
            w.at[p, chip, core, z, :, pl.ds(part * HD, HD)],
            own_sem.at[p, part],
        )

    def sib_weight(p, part):
        ref, col = weight_parts(p, 1 - core)[part]
        return remote(
            ref.at[:, pl.ds(pl.multiple_of(col, HD), HD)],
            w.at[p, chip, core, z, :, pl.ds(part * HD, HD)],
            sib_send.at[p, part], sib_recv.at[p, part], sib,
        )

    def sib_weight_wait(p, part):
        dst = w.at[p, chip, 1 - core, z, :, pl.ds(part * HD, HD)]
        remote(dst, dst, sib_send.at[p, part], sib_recv.at[p, part], sib).wait_recv()

    def z_copy(p, k):
        unit = w.at[p, chip, :, z]
        return remote(unit, unit, z_send.at[p, k - 1], z_recv.at[p, k - 1], None, z_at(k))

    def z_wait(p, k):
        unit = w.at[p, chip, :, z_at(planes - k)]
        remote(unit, unit, z_send.at[p, k - 1], z_recv.at[p, k - 1], None, z_at(k)).wait_recv()

    def x_copy(p, zi, owner):
        unit = w.at[p, owner, :, zi]
        return remote(unit, unit, x_send.at[p, zi], x_recv.at[p, zi], bx)

    def y_copy(p, zi, owner):
        unit = w.at[p, owner, :, zi]
        return remote(unit, unit, y_send.at[p, zi], y_recv.at[p, zi], by)

    def dy_copy(p, zi, owner):
        unit = w.at[p, owner, 0, zi]
        return remote(unit, unit, dy_send.at[p, zi], dy_recv.at[p, zi], by)

    def dx_copy(p, zi, owner):
        unit = w.at[p, owner, 1, zi]
        return remote(unit, unit, dx_send.at[p, zi], dx_recv.at[p, zi], bx)

    def send_column(p, zi):
        x_copy(p, zi, chip).start()
        y_copy(p, zi, chip).start()

    def serve_z(p, k):
        z_wait(p, k)
        send_column(p, z_at(planes - k))

    def serve_diagonal(p, zi):
        x_copy(p, zi, chip_x).wait_recv()
        dy_copy(p, zi, chip_x).start()
        y_copy(p, zi, chip_y).wait_recv()
        dx_copy(p, zi, chip_y).start()

    chip_d = bd // 2

    def plane_copy(k):
        plane = w.at[plane_first, :, :, z]
        return remote(plane, plane, z_send.at[plane_first, k - 1], z_recv.at[plane_first, k - 1], None, z_at(k))

    def arrived(p):
        @pl.when(p < plane_first)
        def _():
            for zi in range(planes):
                dy_copy(p, zi, chip_d).wait_recv()
                dx_copy(p, zi, chip_d).wait_recv()

        @pl.when(p == plane_first)
        def _():
            for k in range(1, planes):
                plane = w.at[plane_first, :, :, z_at(planes - k)]
                remote(
                    plane, plane, z_send.at[plane_first, k - 1], z_recv.at[plane_first, k - 1], None, z_at(k)
                ).wait_recv()

    tokens = (
        (short_ref, pl.multiple_of(core * short_len, short_len), short_len),
        (long_ref, pl.multiple_of(both_short + core * long_count, 128), long_count),
    )
    sib_start = (
        pl.multiple_of((1 - core) * short_len, short_len),
        pl.multiple_of(both_short + (1 - core) * long_count, 128),
    )

    def token_copy(i):
        ref, start, count = tokens[i]
        return pltpu.make_async_copy(ref, x.at[pl.ds(start, count)], tok_sem.at[i])

    def token_remote(i):
        ref, start, count = tokens[i]
        return remote(ref, x.at[pl.ds(start, count)], tok_send.at[i], tok_recv.at[i], sib)

    def token_wait(i):
        dst = x.at[pl.ds(sib_start[i], tokens[i][2])]
        remote(dst, dst, tok_send.at[i], tok_recv.at[i], sib).wait_recv()

    segs = ((segcol_in, segcol), (segrow_in, segrow))

    def seg_copy(i):
        return pltpu.make_async_copy(segs[i][0], segs[i][1].at[core], seg_sem.at[i])

    def seg_remote(i):
        return remote(segs[i][0], segs[i][1].at[core], seg_send.at[i], seg_recv.at[i], sib)

    def seg_wait(i):
        dst = segs[i][1].at[1 - core]
        remote(dst, dst, seg_send.at[i], seg_recv.at[i], sib).wait_recv()

    kv_peers = ((bx, chip_x, cx == 0, cx == 1), (by, chip_y, cy == 0, cy == 1), (bd, chip_d, cy == 0, cy == 1))

    def kv_copy(g, i, owner):
        rows = far_kv.at[g, pl.ds(pl.multiple_of(owner * both_long, 128), both_long)]
        src = proj.at[g, pl.ds(both_short, both_long)]
        return remote(src, rows, kv_send.at[g, i], kv_recv.at[g, i], kv_peers[i][0])

    for p in range(steps):
        for part in range(2):
            own_weight(p, part).start()
            sib_weight(p, part).start()
    for i in range(2):
        seg_copy(i).start()
        seg_remote(i).start()
    for i in range(2):
        token_copy(i).start()
        token_remote(i).start()
    for p in range(steps):
        for part in range(2):
            own_weight(p, part).wait()
            sib_weight_wait(p, part)
        if p < plane_first:
            for k in range(1, planes):
                z_copy(p, k).start()
        send_column(p, z)

    for i in range(2):
        seg_copy(i).wait()
        seg_wait(i)

    block_rows = math.gcd(short_len, 256)
    blocks = [
        (first, max(0, first - LONGEST_DOCUMENT), first + block_rows)
        for first in range(0, short_len, block_rows)
    ]

    @pl.loop(0, 2)
    def _(s):
        for n, (first, low, high) in enumerate(blocks):
            shape = (block_rows, high - low)
            query_pos = first + lax.broadcasted_iota(jnp.int32, shape, 0)
            key_pos = low + lax.broadcasted_iota(jnp.int32, shape, 1)
            visible = (key_pos <= query_pos) & (
                segcol[s, first : first + block_rows, :] == segrow[s, :, low:high]
            )
            bias[s, n, :, : high - low] = jnp.where(visible, 0.0, masked_score)

    def serve_column(p):
        for k in range(1, planes):
            serve_z(p, k)

    def serve_diagonals(p):
        for zi in range(planes):
            serve_diagonal(p, zi)

    serve_column(0)
    serve_diagonals(0)
    serve_diagonal(plane_first, z)
    serve_column(1)
    dy_copy(plane_first, z, chip_d).wait_recv()
    dx_copy(plane_first, z, chip_d).wait_recv()
    for i in range(2):
        token_copy(i).wait()
        token_wait(i)

    row_blocks = (both_short + both_long) // rows_step
    long_block = math.gcd(both_long, 256)
    first_pos = chip * both_long

    def out_copies(q):
        slot = q % 2
        col = pl.multiple_of(core * half_q + q * 2 * HD, HD)
        mine_short = staged.at[slot, pl.ds(tokens[0][1], short_len)]
        mine_long = staged.at[slot, pl.ds(tokens[1][1], long_count)]
        other_short = staged.at[slot, pl.ds(sib_start[0], short_len)]
        other_long = staged.at[slot, pl.ds(sib_start[1], long_count)]
        to_short = short_out.at[:, pl.ds(col, 2 * HD)]
        to_long = long_out.at[:, pl.ds(col, 2 * HD)]
        return (
            pltpu.make_async_copy(mine_short, to_short, out_sem.at[slot, 0]),
            pltpu.make_async_copy(mine_long, to_long, out_sem.at[slot, 1]),
            remote(other_short, to_short, out_send.at[slot, 0], out_recv.at[q, 0], sib),
            remote(other_long, to_long, out_send.at[slot, 1], out_recv.at[q, 1], sib),
        )

    def out_wait_sent(q):
        near_short, near_long, far_short, far_long = out_copies(q)
        near_short.wait()
        near_long.wait()
        far_short.wait_send()
        far_long.wait_send()

    ones = jnp.ones((1, HD), jnp.bfloat16)

    def mix(exponentials, values):
        wide = jnp.concatenate([values, jnp.broadcast_to(ones, values.shape)], axis=1)
        return jnp.dot(exponentials.astype(jnp.bfloat16), wide, preferred_element_type=jnp.float32)

    def two_heads(rows):
        return jnp.concatenate([proj[groups, rows, :HD], proj[groups, rows, HD:]], axis=0)

    def store_heads(slot, rows, result):
        count = result.shape[0] // 2
        staged[slot, rows, :HD] = result[:count]
        staged[slot, rows, HD:] = result[count:]

    def short_pair(g, s, slot):
        base = s * short_len
        for n, (first, low, high) in enumerate(blocks):
            rows = pl.ds(pl.multiple_of(base + first, 128), block_rows)
            keys = pl.ds(pl.multiple_of(base + low, 128), high - low)
            scores = raw_scores(two_heads(rows), proj[g, keys, :HD])
            hidden = bias[s, n, :, : high - low]
            scores = scores + jnp.concatenate([hidden, hidden], axis=0)
            row_max = jnp.max(scores, axis=-1, keepdims=True)
            mixed = mix(jnp.exp2((scores - row_max) * exp2_factor), proj[g, keys, HD:])
            store_heads(slot, rows, (mixed[:, :HD] / mixed[:, HD:]).astype(jnp.bfloat16))

    long_parts = both_long // long_block

    def long_rows(n):
        return pl.ds(both_short + n * long_block, long_block)

    def long_pair(g, slot):
        shape = (long_block, long_block)
        causal = lax.broadcasted_iota(jnp.int32, shape, 1) <= lax.broadcasted_iota(jnp.int32, shape, 0)
        hidden = jnp.where(causal, 0.0, masked_score)
        hidden = jnp.concatenate([hidden, hidden], axis=0)
        for n in range(long_parts):
            seen = (n + 1) * long_block
            keys = pl.ds(both_short, seen)
            scores = raw_scores(two_heads(long_rows(n)), proj[g, keys, :HD])
            last = scores[:, seen - long_block :] + hidden
            if n:
                last = jnp.concatenate([scores[:, : seen - long_block], last], axis=1)
            row_max = jnp.max(last, axis=-1, keepdims=True)
            total[n] = mix(jnp.exp2((last - row_max) * exp2_factor), proj[g, keys, HD:])
            highest[n] = jnp.broadcast_to(row_max, highest.shape[1:])

        @pl.loop(0, chip)
        def _(block):
            far = pl.ds(pl.multiple_of(block * both_long, 128), both_long)
            for n in range(long_parts):
                scores = raw_scores(two_heads(long_rows(n)), far_kv[g, far, :HD])
                old_max = highest[n]
                new_max = jnp.maximum(old_max, jnp.max(scores, axis=-1, keepdims=True))
                rescale = jnp.exp2((old_max - new_max) * exp2_factor)
                exponentials = jnp.exp2((scores - new_max[:, :1]) * exp2_factor)
                added = mix(exponentials, far_kv[g, far, HD:])
                total[n] = total[n] * jnp.concatenate([rescale, rescale], axis=1) + added
                highest[n] = new_max

        long_len = len_ref[core * 0]
        for n in range(long_parts):
            query_pos = first_pos + n * long_block + lax.broadcasted_iota(jnp.int32, (long_block, 1), 0)
            real = jnp.where(query_pos < long_len, 1.0, 0.0)
            mixed = total[n]
            result = jnp.where(jnp.concatenate([real, real], axis=0) > 0.0, mixed[:, :HD] / mixed[:, HD:], 0.0)
            store_heads(slot, long_rows(n), result.astype(jnp.bfloat16))

    @pl.loop(0, steps)
    def _(p):
        g, r = p // per_group, p % per_group
        arrived(p)

        @pl.loop(0, row_blocks)
        def _(i):
            rows = pl.ds(pl.multiple_of(i * rows_step, rows_step), rows_step)
            weights = w[p].reshape(-1, 2 * HD)
            result = jnp.dot(x[rows, :], weights, preferred_element_type=jnp.float32)

            @pl.when(r == 0)
            def _():
                proj[g, rows, :] = result.astype(jnp.bfloat16)

            @pl.when(r > 0)
            def _():
                proj[groups, rows, :] = result.astype(jnp.bfloat16)

        @pl.when(p + 1 < plane_first)
        def _():
            serve_diagonals(p + 1)

        @pl.when(r == 0)
        def _():
            for n, (_, _, sends, _) in enumerate(kv_peers):
                @pl.when(sends)
                def _():
                    kv_copy(g, n, chip).start()

        @pl.when(p == 0)
        def _():
            serve_column(2)

        @pl.when(p + 3 < plane_first)
        def _():
            serve_column(p + 3)

        @pl.when(p + 4 == plane_first)
        def _():
            for k in range(1, planes):
                plane_copy(k).start()

        @pl.when(r > 0)
        def _():
            q = g * pairs + r - 1
            slot = q % 2

            @pl.when(q >= 2)
            def _():
                out_wait_sent(q - 2)

            @pl.loop(0, 2)
            def _(s):
                short_pair(g, s, slot)

            @pl.when(r == 1)
            def _():
                for n, (_, owner, _, receives) in enumerate(kv_peers):
                    @pl.when(receives)
                    def _():
                        kv_copy(g, n, owner).wait_recv()

            long_pair(g, slot)

            for copy in out_copies(q):
                copy.start()

    total_q = groups * pairs

    @pl.loop(max(0, total_q - 2), total_q)
    def _(q):
        out_wait_sent(q)

    @pl.loop(0, total_q)
    def _(q):
        _, _, far_short, far_long = out_copies(q)
        far_short.wait_recv()
        far_long.wait_recv()

    for p in range(steps):
        for part in range(2):
            sib_weight(p, part).wait_send()

    for k in range(1, planes):
        plane_copy(k).wait_send()
    x_copy(plane_first, z, chip).wait_send()
    y_copy(plane_first, z, chip).wait_send()
    dy_copy(plane_first, z, chip_x).wait_send()
    dx_copy(plane_first, z, chip_y).wait_send()

    @pl.loop(0, plane_first)
    def _(p):
        for k in range(1, planes):
            z_copy(p, k).wait_send()
        for zi in range(planes):
            x_copy(p, zi, chip).wait_send()
            y_copy(p, zi, chip).wait_send()
            dy_copy(p, zi, chip_x).wait_send()
            dx_copy(p, zi, chip_y).wait_send()

    for i in range(2):
        token_remote(i).wait_send()
        seg_remote(i).wait_send()
    for g in range(groups):
        for n, (_, _, sends, _) in enumerate(kv_peers):
            @pl.when(sends)
            def _():
                kv_copy(g, n, chip).wait_send()


def fused_local(planes, short_tokens, short_segments, long_tokens, long_lengths, w_query, w_key, w_value):
    short_rows, long_rows, segments = short_tokens[0], long_tokens[0], short_segments[0]
    short_len, width = short_rows.shape
    long_count = long_rows.shape[0]
    heads, kv_heads = w_query.shape[1] // HD, w_key.shape[1] // HD
    groups, pairs = kv_heads // 2, heads // kv_heads // 2
    steps = groups * (1 + pairs)
    depth = w_query.shape[0]
    chips = width // (depth * 2 * planes)
    total_rows = 2 * (short_len + long_count)
    rows_step = math.gcd(total_rows, 1408)
    block_rows = math.gcd(short_len, 256)
    long_block = math.gcd(2 * long_count, 256)
    widest = min(short_len, LONGEST_DOCUMENT + block_rows)
    dims = (planes, short_len, long_count, groups, pairs, rows_step)
    dma = pltpu.SemaphoreType.DMA
    bf16 = jnp.bfloat16
    any_space = pl.BlockSpec(memory_space=pl.ANY)
    short, long = pl.pallas_call(
        functools.partial(fused_kernel, dims),
        in_specs=[pl.BlockSpec(memory_space=pltpu.SMEM)] + [any_space] * 7,
        out_specs=[any_space] * 2,
        out_shape=[
            jax.ShapeDtypeStruct((short_len, heads * HD), bf16),
            jax.ShapeDtypeStruct((long_count, heads * HD), bf16),
        ],
        scratch_shapes=[
            pltpu.VMEM((total_rows, width), bf16),
            pltpu.VMEM((steps, chips, 2, planes, depth, 2 * HD), bf16),
            pltpu.VMEM((groups + 1, total_rows, 2 * HD), bf16),
            pltpu.VMEM((groups, chips * 2 * long_count, 2 * HD), bf16),
            pltpu.VMEM((2, short_len // block_rows, block_rows, widest), jnp.float32),
            pltpu.VMEM((2, total_rows, 2 * HD), bf16),
            pltpu.VMEM((2, short_len, 1), jnp.int32),
            pltpu.VMEM((2, 1, short_len), jnp.int32),
            dma((steps, planes - 1)), dma((steps, planes - 1)),
            dma((steps, planes)), dma((steps, planes)),
            dma((steps, planes)), dma((steps, planes)),
            dma((steps, planes)), dma((steps, planes)),
            dma((steps, planes)), dma((steps, planes)),
            dma((steps, 2)), dma((steps, 2)), dma((steps, 2)),
            dma((2,)), dma((2,)), dma((2,)),
            dma((2,)), dma((2,)), dma((2,)),
            dma((groups, 3)), dma((groups, 3)),
            dma((2, 2)), dma((2, 2)), dma((groups * pairs, 2)),
            pltpu.VMEM((2 * long_count // long_block, 2 * long_block, 2 * HD), jnp.float32),
            pltpu.VMEM((2 * long_count // long_block, 2 * long_block, HD), jnp.float32),
        ],
        compiler_params=pltpu.CompilerParams(
            collective_id=0, has_side_effects=True, vmem_limit_bytes=67043328
        ),
    )(long_lengths, segments[:, None], segments[None, :], short_rows, long_rows, w_query, w_key, w_value)
    return short[None], long[None]


def solution(mesh):
    planes = mesh.shape["dp"]
    fused = mesh.shape["blk"] == 8 and mesh.shape["uly"] == 1 and planes > 1
    return jax.shard_map(
        functools.partial(fused_local, planes) if fused else local,
        mesh=mesh,
        in_specs=(
            P(("blk", "dp"), "uly", None),
            P(("blk", "dp"), None),
            P("dp", "blk", None),
            P("dp"),
            P(("blk", "dp"), "uly"),
            P(("blk", "dp"), "uly"),
            P(("blk", "dp"), "uly"),
        ),
        out_specs=(P(("blk", "dp"), "uly", None), P("dp", "blk", "uly")),
        check_vma=False,
    )
```

```python
import functools
import math

import jax
import jax.numpy as jnp
from jax import lax
from jax.experimental import pallas as pl
from jax.experimental.pallas import tpu as pltpu
from jax.sharding import PartitionSpec as P

HD = 128
LONGEST_DOCUMENT = 512

masked_score = -1e30
exp2_factor = math.log2(math.e) / math.sqrt(HD)


def raw_scores(queries, keys):
    return lax.dot_general(
        queries, keys, (((1,), (1,)), ((), ())), preferred_element_type=jnp.float32
    )


def short_kernel(block_rows, col_ref, row_ref, q_ref, k_ref, v_ref, out_ref, bias_ref):
    seq_len = q_ref.shape[0]

    def window(first_row):
        return max(0, first_row - LONGEST_DOCUMENT), first_row + block_rows

    @pl.when(pl.program_id(0) == 0)
    def _():
        for first_row in range(0, seq_len, block_rows):
            low, high = window(first_row)
            shape = (block_rows, high - low)
            query_pos = first_row + lax.broadcasted_iota(jnp.int32, shape, 0)
            key_pos = low + lax.broadcasted_iota(jnp.int32, shape, 1)
            visible = (key_pos <= query_pos) & (
                col_ref[first_row : first_row + block_rows, :] == row_ref[:, low:high]
            )
            bias_ref[first_row : first_row + block_rows, low:high] = jnp.where(
                visible, 0.0, masked_score
            )

    for first_row in range(0, seq_len, block_rows):
        low, high = window(first_row)
        rows = slice(first_row, first_row + block_rows)
        scores = raw_scores(q_ref[rows, :], k_ref[low:high, :]) + bias_ref[rows, low:high]
        row_max = jnp.max(scores, axis=-1, keepdims=True)
        exponentials = jnp.exp2((scores - row_max) * exp2_factor)
        totals = jnp.sum(exponentials, axis=-1, keepdims=True)
        mixed = jnp.dot(
            exponentials.astype(jnp.bfloat16),
            v_ref[low:high, :],
            preferred_element_type=jnp.float32,
        )
        out_ref[rows, :] = (mixed / totals).astype(jnp.bfloat16)


def short_attention(projected, segments, heads, kv_heads):
    seq_len = projected.shape[0]
    group = heads // kv_heads
    block_rows = math.gcd(seq_len, 256)
    return pl.pallas_call(
        functools.partial(short_kernel, block_rows),
        grid=(heads,),
        in_specs=[
            pl.BlockSpec((seq_len, 1), lambda h: (0, 0)),
            pl.BlockSpec((1, seq_len), lambda h: (0, 0)),
            pl.BlockSpec((seq_len, HD), lambda h: (0, h)),
            pl.BlockSpec((seq_len, HD), lambda h: (0, heads + h // group)),
            pl.BlockSpec((seq_len, HD), lambda h: (0, heads + kv_heads + h // group)),
        ],
        out_specs=pl.BlockSpec((seq_len, HD), lambda h: (0, h)),
        out_shape=jax.ShapeDtypeStruct((seq_len, heads * HD), jnp.bfloat16),
        scratch_shapes=[pltpu.VMEM((seq_len, seq_len), jnp.float32)],
        cost_estimate=pl.CostEstimate(
            flops=4 * heads * seq_len * seq_len * HD,
            bytes_accessed=4 * seq_len * heads * HD,
            transcendentals=heads * seq_len * seq_len,
        ),
        compiler_params=pltpu.CompilerParams(dimension_semantics=("arbitrary",)),
    )(segments[:, None], segments[None, :], projected, projected, projected)


def long_kernel(key_rows, info_ref, q_ref, k_ref, v_ref, out_ref):
    long_count = q_ref.shape[0]
    first_pos = info_ref[0]
    long_len = info_ref[1]
    queries = q_ref[...]
    query_pos = first_pos + lax.broadcasted_iota(jnp.int32, (long_count, 1), 0)
    last_key = jnp.minimum(query_pos, long_len - 1)

    def update(block, states, masked):
        running_max, running_sum, accumulated = states
        start = pl.multiple_of(block * key_rows, key_rows)
        scores = raw_scores(queries, k_ref[pl.ds(start, key_rows), :])
        if masked:
            key_pos = start + lax.broadcasted_iota(jnp.int32, (long_count, key_rows), 1)
            scores = jnp.where(key_pos <= last_key, scores, masked_score)
        new_max = jnp.maximum(running_max, jnp.max(scores, axis=-1, keepdims=True))
        rescale = jnp.exp2((running_max - new_max) * exp2_factor)
        exponentials = jnp.exp2((scores - new_max) * exp2_factor)
        running_sum = running_sum * rescale + jnp.sum(exponentials, axis=-1, keepdims=True)
        accumulated = accumulated * rescale + jnp.dot(
            exponentials.astype(jnp.bfloat16),
            v_ref[pl.ds(start, key_rows), :],
            preferred_element_type=jnp.float32,
        )
        return new_max, running_sum, accumulated

    @pl.when(first_pos >= long_len)
    def _():
        out_ref[...] = jnp.zeros_like(out_ref)

    @pl.when(first_pos < long_len)
    def _():
        whole = jnp.minimum(first_pos + 1, long_len) // key_rows
        used = (jnp.minimum(first_pos + long_count, long_len) + key_rows - 1) // key_rows
        states = (
            jnp.full((long_count, 1), masked_score, jnp.float32),
            jnp.zeros((long_count, 1), jnp.float32),
            jnp.zeros((long_count, HD), jnp.float32),
        )
        states = lax.fori_loop(0, whole, lambda i, s: update(i, s, False), states)
        states = lax.fori_loop(whole, used, lambda i, s: update(i, s, True), states)
        running_max, running_sum, accumulated = states
        mixed = jnp.where(query_pos < long_len, accumulated / running_sum, 0.0)
        out_ref[...] = mixed.astype(jnp.bfloat16)


def long_attention(queries, kv_rows, first_pos, long_len, kv_heads):
    long_count = queries.shape[0]
    heads = queries.shape[1] // HD
    total_rows = kv_rows.shape[0]
    group = heads // kv_heads
    key_rows = math.gcd(total_rows, 768)
    return pl.pallas_call(
        functools.partial(long_kernel, key_rows),
        grid_spec=pltpu.PrefetchScalarGridSpec(
            num_scalar_prefetch=1,
            grid=(heads,),
            in_specs=[
                pl.BlockSpec((long_count, HD), lambda h, info: (0, h)),
                pl.BlockSpec((total_rows, HD), lambda h, info: (0, h // group)),
                pl.BlockSpec((total_rows, HD), lambda h, info: (0, kv_heads + h // group)),
            ],
            out_specs=pl.BlockSpec((long_count, HD), lambda h, info: (0, h)),
        ),
        out_shape=jax.ShapeDtypeStruct((long_count, heads * HD), jnp.bfloat16),
        cost_estimate=pl.CostEstimate(
            flops=4 * heads * long_count * total_rows * HD,
            bytes_accessed=4 * total_rows * kv_heads * HD,
            transcendentals=heads * long_count * total_rows,
        ),
        compiler_params=pltpu.CompilerParams(dimension_semantics=("arbitrary",)),
    )(jnp.stack([first_pos, long_len]), queries, kv_rows, kv_rows)


def project(rows, weight):
    return jnp.dot(rows, weight, preferred_element_type=jnp.float32).astype(jnp.bfloat16)


def local(short_tokens, short_segments, long_tokens, long_lengths, w_query, w_key, w_value):
    short_rows = short_tokens[0]
    long_rows = long_tokens[0]
    long_count = long_rows.shape[0]
    query_cols = w_query.shape[1]
    heads, kv_heads = query_cols // HD, w_key.shape[1] // HD
    weights = lax.all_gather(
        jnp.concatenate([w_query, w_key, w_value], axis=1), ("blk", "dp"), axis=0, tiled=True
    )
    kv_long = project(long_rows, weights[:, query_cols:])
    kv_whole = lax.all_gather(kv_long, "blk", axis=0, tiled=True)
    whole_rows = lax.all_gather(short_rows, "uly", axis=0, tiled=True)
    short_projected = project(whole_rows, weights)
    query_long = project(long_rows, weights[:, :query_cols])
    attended = short_attention(short_projected, short_segments[0], heads, kv_heads)
    short_back = lax.all_to_all(attended, "uly", split_axis=0, concat_axis=1, tiled=True)
    first_pos = lax.axis_index("blk").astype(jnp.int32) * long_count
    mixed = long_attention(query_long, kv_whole, first_pos, long_lengths[0], kv_heads)
    return short_back[None], mixed[None]


MESH = pl.DeviceIdType.MESH


def fused_kernel(
    dims, len_ref, segcol_in, segrow_in, short_ref, long_ref, wq_ref, wk_ref, wv_ref,
    short_out, long_out,
    x, w, proj, far_kv, bias, staged, segcol, segrow,
    z_send, z_recv, x_send, x_recv, y_send, y_recv, dx_send, dx_recv, dy_send, dy_recv,
    own_sem, sib_send, sib_recv, tok_sem, tok_send, tok_recv, seg_sem, seg_send, seg_recv,
    kv_send, kv_recv, out_sem, out_send, out_recv, total, highest,
):
    planes, short_len, long_count, groups, pairs, rows_step = dims
    per_group = 1 + pairs
    steps = groups * per_group
    plane_first = steps - 1
    both_short, both_long = 2 * short_len, 2 * long_count
    half_q, half_kv = groups * pairs * 2 * HD, groups * HD

    b, z = lax.axis_index("blk"), lax.axis_index("dp")
    core, chip = b % 2, b // 2
    cx, cy = chip % 2, chip // 2
    sib = b + 1 - 2 * core
    bx = b + 2 - 4 * cx
    by = b + 4 - 8 * cy
    bd = bx + by - b
    chip_x, chip_y = bx // 2, by // 2

    def z_at(k):
        return (z + k) % planes

    def remote(src, dst, send, recv, blk, dp=None):
        where = {"blk": blk} if dp is None else {"dp": dp}
        return pltpu.make_async_remote_copy(
            src_ref=src, dst_ref=dst, send_sem=send, recv_sem=recv,
            device_id=where, device_id_type=MESH,
        )

    barrier = pltpu.get_barrier_semaphore()
    for peer in (sib, bx, by, bd):
        pl.semaphore_signal(barrier, inc=1, device_id={"blk": peer}, device_id_type=MESH)
    for k in range(1, planes):
        pl.semaphore_signal(barrier, inc=1, device_id={"dp": z_at(k)}, device_id_type=MESH)
    pl.semaphore_wait(barrier, 4 + planes - 1)

    def weight_parts(p, half):
        g, r = p // per_group, p % per_group
        if r == 0:
            return ((wk_ref, half * half_kv + g * HD), (wv_ref, half * half_kv + g * HD))
        q = half * half_q + (g * pairs + r - 1) * 2 * HD
        return ((wq_ref, q), (wq_ref, q + HD))

    def own_weight(p, part):
        ref, col = weight_parts(p, core)[part]
        return pltpu.make_async_copy(
            ref.at[:, pl.ds(pl.multiple_of(col, HD), HD)],
            w.at[p, chip, core, z, :, pl.ds(part * HD, HD)],
            own_sem.at[p, part],
        )

    def sib_weight(p, part):
        ref, col = weight_parts(p, 1 - core)[part]
        return remote(
            ref.at[:, pl.ds(pl.multiple_of(col, HD), HD)],
            w.at[p, chip, core, z, :, pl.ds(part * HD, HD)],
            sib_send.at[p, part], sib_recv.at[p, part], sib,
        )

    def sib_weight_wait(p, part):
        dst = w.at[p, chip, 1 - core, z, :, pl.ds(part * HD, HD)]
        remote(dst, dst, sib_send.at[p, part], sib_recv.at[p, part], sib).wait_recv()

    def z_copy(p, k):
        unit = w.at[p, chip, :, z]
        return remote(unit, unit, z_send.at[p, k - 1], z_recv.at[p, k - 1], None, z_at(k))

    def z_wait(p, k):
        unit = w.at[p, chip, :, z_at(planes - k)]
        remote(unit, unit, z_send.at[p, k - 1], z_recv.at[p, k - 1], None, z_at(k)).wait_recv()

    def x_copy(p, zi, owner):
        unit = w.at[p, owner, :, zi]
        return remote(unit, unit, x_send.at[p, zi], x_recv.at[p, zi], bx)

    def y_copy(p, zi, owner):
        unit = w.at[p, owner, :, zi]
        return remote(unit, unit, y_send.at[p, zi], y_recv.at[p, zi], by)

    def dy_copy(p, zi, owner):
        unit = w.at[p, owner, 0, zi]
        return remote(unit, unit, dy_send.at[p, zi], dy_recv.at[p, zi], by)

    def dx_copy(p, zi, owner):
        unit = w.at[p, owner, 1, zi]
        return remote(unit, unit, dx_send.at[p, zi], dx_recv.at[p, zi], bx)

    def send_column(p, zi):
        x_copy(p, zi, chip).start()
        y_copy(p, zi, chip).start()

    def serve_z(p, k):
        z_wait(p, k)
        send_column(p, z_at(planes - k))

    def serve_diagonal(p, zi):
        x_copy(p, zi, chip_x).wait_recv()
        dy_copy(p, zi, chip_x).start()
        y_copy(p, zi, chip_y).wait_recv()
        dx_copy(p, zi, chip_y).start()

    chip_d = bd // 2

    def plane_copy(k):
        plane = w.at[plane_first, :, :, z]
        return remote(plane, plane, z_send.at[plane_first, k - 1], z_recv.at[plane_first, k - 1], None, z_at(k))

    def arrived(p):
        @pl.when(p < plane_first)
        def _():
            for zi in range(planes):
                dy_copy(p, zi, chip_d).wait_recv()
                dx_copy(p, zi, chip_d).wait_recv()

        @pl.when(p == plane_first)
        def _():
            for k in range(1, planes):
                plane = w.at[plane_first, :, :, z_at(planes - k)]
                remote(
                    plane, plane, z_send.at[plane_first, k - 1], z_recv.at[plane_first, k - 1], None, z_at(k)
                ).wait_recv()

    tokens = (
        (short_ref, pl.multiple_of(core * short_len, short_len), short_len),
        (long_ref, pl.multiple_of(both_short + core * long_count, 128), long_count),
    )
    sib_start = (
        pl.multiple_of((1 - core) * short_len, short_len),
        pl.multiple_of(both_short + (1 - core) * long_count, 128),
    )

    def token_copy(i):
        ref, start, count = tokens[i]
        return pltpu.make_async_copy(ref, x.at[pl.ds(start, count)], tok_sem.at[i])

    def token_remote(i):
        ref, start, count = tokens[i]
        return remote(ref, x.at[pl.ds(start, count)], tok_send.at[i], tok_recv.at[i], sib)

    def token_wait(i):
        dst = x.at[pl.ds(sib_start[i], tokens[i][2])]
        remote(dst, dst, tok_send.at[i], tok_recv.at[i], sib).wait_recv()

    segs = ((segcol_in, segcol), (segrow_in, segrow))

    def seg_copy(i):
        return pltpu.make_async_copy(segs[i][0], segs[i][1].at[core], seg_sem.at[i])

    def seg_remote(i):
        return remote(segs[i][0], segs[i][1].at[core], seg_send.at[i], seg_recv.at[i], sib)

    def seg_wait(i):
        dst = segs[i][1].at[1 - core]
        remote(dst, dst, seg_send.at[i], seg_recv.at[i], sib).wait_recv()

    kv_peers = ((bx, chip_x, cx == 0, cx == 1), (by, chip_y, cy == 0, cy == 1), (bd, chip_d, cy == 0, cy == 1))

    def kv_copy(g, i, owner):
        rows = far_kv.at[g, pl.ds(pl.multiple_of(owner * both_long, 128), both_long)]
        src = proj.at[g, pl.ds(both_short, both_long)]
        return remote(src, rows, kv_send.at[g, i], kv_recv.at[g, i], kv_peers[i][0])

    for p in range(steps):
        for part in range(2):
            own_weight(p, part).start()
            sib_weight(p, part).start()
    for i in range(2):
        seg_copy(i).start()
        seg_remote(i).start()
    for i in range(2):
        token_copy(i).start()
        token_remote(i).start()
    for p in range(steps):
        for part in range(2):
            own_weight(p, part).wait()
            sib_weight_wait(p, part)
        if p < plane_first:
            for k in range(1, planes):
                z_copy(p, k).start()
        send_column(p, z)

    for i in range(2):
        seg_copy(i).wait()
        seg_wait(i)

    block_rows = math.gcd(short_len, 256)
    blocks = [
        (first, max(0, first - LONGEST_DOCUMENT), first + block_rows)
        for first in range(0, short_len, block_rows)
    ]

    @pl.loop(0, 2)
    def _(s):
        for n, (first, low, high) in enumerate(blocks):
            shape = (block_rows, high - low)
            query_pos = first + lax.broadcasted_iota(jnp.int32, shape, 0)
            key_pos = low + lax.broadcasted_iota(jnp.int32, shape, 1)
            visible = (key_pos <= query_pos) & (
                segcol[s, first : first + block_rows, :] == segrow[s, :, low:high]
            )
            bias[s, n, :, : high - low] = jnp.where(visible, 0.0, masked_score)

    def serve_column(p):
        for k in range(1, planes):
            serve_z(p, k)

    def serve_diagonals(p):
        for zi in range(planes):
            serve_diagonal(p, zi)

    serve_column(0)
    serve_diagonals(0)
    serve_diagonal(plane_first, z)
    serve_column(1)
    dy_copy(plane_first, z, chip_d).wait_recv()
    dx_copy(plane_first, z, chip_d).wait_recv()
    for i in range(2):
        token_copy(i).wait()
        token_wait(i)

    row_blocks = (both_short + both_long) // rows_step
    long_block = math.gcd(both_long, 256)
    first_pos = chip * both_long

    def out_copies(q):
        slot = q % 2
        col = pl.multiple_of(core * half_q + q * 2 * HD, HD)
        mine_short = staged.at[slot, pl.ds(tokens[0][1], short_len)]
        mine_long = staged.at[slot, pl.ds(tokens[1][1], long_count)]
        other_short = staged.at[slot, pl.ds(sib_start[0], short_len)]
        other_long = staged.at[slot, pl.ds(sib_start[1], long_count)]
        to_short = short_out.at[:, pl.ds(col, 2 * HD)]
        to_long = long_out.at[:, pl.ds(col, 2 * HD)]
        return (
            pltpu.make_async_copy(mine_short, to_short, out_sem.at[slot, 0]),
            pltpu.make_async_copy(mine_long, to_long, out_sem.at[slot, 1]),
            remote(other_short, to_short, out_send.at[slot, 0], out_recv.at[q, 0], sib),
            remote(other_long, to_long, out_send.at[slot, 1], out_recv.at[q, 1], sib),
        )

    def out_wait_sent(q):
        near_short, near_long, far_short, far_long = out_copies(q)
        near_short.wait()
        near_long.wait()
        far_short.wait_send()
        far_long.wait_send()

    ones = jnp.ones((1, HD), jnp.bfloat16)

    def mix(exponentials, values):
        wide = jnp.concatenate([values, jnp.broadcast_to(ones, values.shape)], axis=1)
        return jnp.dot(exponentials.astype(jnp.bfloat16), wide, preferred_element_type=jnp.float32)

    def two_heads(rows):
        return jnp.concatenate([proj[groups, rows, :HD], proj[groups, rows, HD:]], axis=0)

    def store_heads(slot, rows, result):
        count = result.shape[0] // 2
        staged[slot, rows, :HD] = result[:count]
        staged[slot, rows, HD:] = result[count:]

    def short_pair(g, s, slot):
        base = s * short_len
        for n, (first, low, high) in enumerate(blocks):
            rows = pl.ds(pl.multiple_of(base + first, 128), block_rows)
            keys = pl.ds(pl.multiple_of(base + low, 128), high - low)
            scores = raw_scores(two_heads(rows), proj[g, keys, :HD])
            hidden = bias[s, n, :, : high - low]
            scores = scores + jnp.concatenate([hidden, hidden], axis=0)
            row_max = jnp.max(scores, axis=-1, keepdims=True)
            mixed = mix(jnp.exp2((scores - row_max) * exp2_factor), proj[g, keys, HD:])
            store_heads(slot, rows, (mixed[:, :HD] / mixed[:, HD:]).astype(jnp.bfloat16))

    long_parts = both_long // long_block

    def long_rows(n):
        return pl.ds(both_short + n * long_block, long_block)

    def long_pair(g, slot):
        shape = (long_block, long_block)
        causal = lax.broadcasted_iota(jnp.int32, shape, 1) <= lax.broadcasted_iota(jnp.int32, shape, 0)
        hidden = jnp.where(causal, 0.0, masked_score)
        hidden = jnp.concatenate([hidden, hidden], axis=0)
        for n in range(long_parts):
            seen = (n + 1) * long_block
            keys = pl.ds(both_short, seen)
            scores = raw_scores(two_heads(long_rows(n)), proj[g, keys, :HD])
            last = scores[:, seen - long_block :] + hidden
            if n:
                last = jnp.concatenate([scores[:, : seen - long_block], last], axis=1)
            row_max = jnp.max(last, axis=-1, keepdims=True)
            total[n] = mix(jnp.exp2((last - row_max) * exp2_factor), proj[g, keys, HD:])
            highest[n] = jnp.broadcast_to(row_max, highest.shape[1:])

        @pl.loop(0, chip)
        def _(block):
            far = pl.ds(pl.multiple_of(block * both_long, 128), both_long)
            for n in range(long_parts):
                scores = raw_scores(two_heads(long_rows(n)), far_kv[g, far, :HD])
                old_max = highest[n]
                new_max = jnp.maximum(old_max, jnp.max(scores, axis=-1, keepdims=True))
                rescale = jnp.exp2((old_max - new_max) * exp2_factor)
                exponentials = jnp.exp2((scores - new_max[:, :1]) * exp2_factor)
                added = mix(exponentials, far_kv[g, far, HD:])
                total[n] = total[n] * jnp.concatenate([rescale, rescale], axis=1) + added
                highest[n] = new_max

        long_len = len_ref[core * 0]
        for n in range(long_parts):
            query_pos = first_pos + n * long_block + lax.broadcasted_iota(jnp.int32, (long_block, 1), 0)
            real = jnp.where(query_pos < long_len, 1.0, 0.0)
            mixed = total[n]
            result = jnp.where(jnp.concatenate([real, real], axis=0) > 0.0, mixed[:, :HD] / mixed[:, HD:], 0.0)
            store_heads(slot, long_rows(n), result.astype(jnp.bfloat16))

    @pl.loop(0, steps)
    def _(p):
        g, r = p // per_group, p % per_group
        arrived(p)

        @pl.when((p >= 2) & (p + 1 < plane_first))
        def _():
            serve_diagonals(p + 1)

        @pl.loop(0, row_blocks)
        def _(i):
            rows = pl.ds(pl.multiple_of(i * rows_step, rows_step), rows_step)
            weights = w[p].reshape(-1, 2 * HD)
            result = jnp.dot(x[rows, :], weights, preferred_element_type=jnp.float32)

            @pl.when(r == 0)
            def _():
                proj[g, rows, :] = result.astype(jnp.bfloat16)

            @pl.when(r > 0)
            def _():
                proj[groups, rows, :] = result.astype(jnp.bfloat16)

        @pl.when((p < 2) & (p + 1 < plane_first))
        def _():
            serve_diagonals(p + 1)

        @pl.when(r == 0)
        def _():
            for n, (_, _, sends, _) in enumerate(kv_peers):
                @pl.when(sends)
                def _():
                    kv_copy(g, n, chip).start()

        @pl.when(p == 0)
        def _():
            serve_column(2)

        @pl.when(p + 3 < plane_first)
        def _():
            serve_column(p + 3)

        @pl.when(p + 4 == plane_first)
        def _():
            for k in range(1, planes):
                plane_copy(k).start()

        @pl.when(r > 0)
        def _():
            q = g * pairs + r - 1
            slot = q % 2

            @pl.when(q >= 2)
            def _():
                out_wait_sent(q - 2)

            @pl.loop(0, 2)
            def _(s):
                short_pair(g, s, slot)

            @pl.when(r == 1)
            def _():
                for n, (_, owner, _, receives) in enumerate(kv_peers):
                    @pl.when(receives)
                    def _():
                        kv_copy(g, n, owner).wait_recv()

            long_pair(g, slot)

            for copy in out_copies(q):
                copy.start()

    total_q = groups * pairs

    @pl.loop(max(0, total_q - 2), total_q)
    def _(q):
        out_wait_sent(q)

    @pl.loop(0, total_q)
    def _(q):
        _, _, far_short, far_long = out_copies(q)
        far_short.wait_recv()
        far_long.wait_recv()

    for p in range(steps):
        for part in range(2):
            sib_weight(p, part).wait_send()

    for k in range(1, planes):
        plane_copy(k).wait_send()
    x_copy(plane_first, z, chip).wait_send()
    y_copy(plane_first, z, chip).wait_send()
    dy_copy(plane_first, z, chip_x).wait_send()
    dx_copy(plane_first, z, chip_y).wait_send()

    @pl.loop(0, plane_first)
    def _(p):
        for k in range(1, planes):
            z_copy(p, k).wait_send()
        for zi in range(planes):
            x_copy(p, zi, chip).wait_send()
            y_copy(p, zi, chip).wait_send()
            dy_copy(p, zi, chip_x).wait_send()
            dx_copy(p, zi, chip_y).wait_send()

    for i in range(2):
        token_remote(i).wait_send()
        seg_remote(i).wait_send()
    for g in range(groups):
        for n, (_, _, sends, _) in enumerate(kv_peers):
            @pl.when(sends)
            def _():
                kv_copy(g, n, chip).wait_send()


def fused_local(planes, short_tokens, short_segments, long_tokens, long_lengths, w_query, w_key, w_value):
    short_rows, long_rows, segments = short_tokens[0], long_tokens[0], short_segments[0]
    short_len, width = short_rows.shape
    long_count = long_rows.shape[0]
    heads, kv_heads = w_query.shape[1] // HD, w_key.shape[1] // HD
    groups, pairs = kv_heads // 2, heads // kv_heads // 2
    steps = groups * (1 + pairs)
    depth = w_query.shape[0]
    chips = width // (depth * 2 * planes)
    total_rows = 2 * (short_len + long_count)
    rows_step = math.gcd(total_rows, 1408)
    block_rows = math.gcd(short_len, 256)
    long_block = math.gcd(2 * long_count, 256)
    widest = min(short_len, LONGEST_DOCUMENT + block_rows)
    dims = (planes, short_len, long_count, groups, pairs, rows_step)
    dma = pltpu.SemaphoreType.DMA
    bf16 = jnp.bfloat16
    any_space = pl.BlockSpec(memory_space=pl.ANY)
    short, long = pl.pallas_call(
        functools.partial(fused_kernel, dims),
        in_specs=[pl.BlockSpec(memory_space=pltpu.SMEM)] + [any_space] * 7,
        out_specs=[any_space] * 2,
        out_shape=[
            jax.ShapeDtypeStruct((short_len, heads * HD), bf16),
            jax.ShapeDtypeStruct((long_count, heads * HD), bf16),
        ],
        scratch_shapes=[
            pltpu.VMEM((total_rows, width), bf16),
            pltpu.VMEM((steps, chips, 2, planes, depth, 2 * HD), bf16),
            pltpu.VMEM((groups + 1, total_rows, 2 * HD), bf16),
            pltpu.VMEM((groups, chips * 2 * long_count, 2 * HD), bf16),
            pltpu.VMEM((2, short_len // block_rows, block_rows, widest), jnp.float32),
            pltpu.VMEM((2, total_rows, 2 * HD), bf16),
            pltpu.VMEM((2, short_len, 1), jnp.int32),
            pltpu.VMEM((2, 1, short_len), jnp.int32),
            dma((steps, planes - 1)), dma((steps, planes - 1)),
            dma((steps, planes)), dma((steps, planes)),
            dma((steps, planes)), dma((steps, planes)),
            dma((steps, planes)), dma((steps, planes)),
            dma((steps, planes)), dma((steps, planes)),
            dma((steps, 2)), dma((steps, 2)), dma((steps, 2)),
            dma((2,)), dma((2,)), dma((2,)),
            dma((2,)), dma((2,)), dma((2,)),
            dma((groups, 3)), dma((groups, 3)),
            dma((2, 2)), dma((2, 2)), dma((groups * pairs, 2)),
            pltpu.VMEM((2 * long_count // long_block, 2 * long_block, 2 * HD), jnp.float32),
            pltpu.VMEM((2 * long_count // long_block, 2 * long_block, HD), jnp.float32),
        ],
        compiler_params=pltpu.CompilerParams(
            collective_id=0, has_side_effects=True, vmem_limit_bytes=67043328
        ),
    )(long_lengths, segments[:, None], segments[None, :], short_rows, long_rows, w_query, w_key, w_value)
    return short[None], long[None]


def solution(mesh):
    planes = mesh.shape["dp"]
    fused = mesh.shape["blk"] == 8 and mesh.shape["uly"] == 1 and planes > 1
    return jax.shard_map(
        functools.partial(fused_local, planes) if fused else local,
        mesh=mesh,
        in_specs=(
            P(("blk", "dp"), "uly", None),
            P(("blk", "dp"), None),
            P("dp", "blk", None),
            P("dp"),
            P(("blk", "dp"), "uly"),
            P(("blk", "dp"), "uly"),
            P(("blk", "dp"), "uly"),
        ),
        out_specs=(P(("blk", "dp"), "uly", None), P("dp", "blk", "uly")),
        check_vma=False,
    )
```
